256 devices in a mesh: section: 4 (over x_hi, core), dp: 64 (over y, x_lo, z).
Axes of the slice: x: 4 (x_hi: 2, x_lo: 2; x = x_hi * 2 + x_lo), y: 4, z: 8, core: 2. Of those that a mesh axis runs over, the one named last changes fastest.
Arguments:
- activations: bfloat16 [12288, 8, 4096], P('dp', 'section'), may hold values from -8 to 8
- damping: float32 [8], P('section'), may hold values from 0.1 to 1
Outputs:
- schur_inverse: float32 [256, 128, 128], P(('section', 'dp'))
- coupling: float32 [256, 128, 128], P(('section', 'dp'))
The draws below stay inside these ranges and needn't reach their ends.
All inputs are finite; a program needn't handle non-finite values.
Results may differ from the reference program's by a relative error of at most 0.0003.
Values may be sent and summed in bfloat16 or wider, within the bound.
A program may use at most 64 MiB of HBM per device.

```python
import math
from functools import partial
import jax
import jax.numpy as jnp
from jax import lax

D = 4096
B = 128
TOK_DEV = 192
L = 8
NB = 32
TOKENS = 12288


def column_filter():
    rows_idx = jnp.arange(B)[:, None]
    cols_idx = jnp.arange(B)[None, :]
    lag_power = jnp.maximum(rows_idx - cols_idx, 0).astype(jnp.float32)
    fresh_weight = jnp.where(cols_idx == 0, 1.0, jnp.sqrt(1.0 - 0.9 * 0.9)).astype(jnp.float32)
    weights = jnp.power(jnp.float32(0.9), lag_power) * fresh_weight
    return jnp.where(rows_idx >= cols_idx, weights, 0.0).astype(jnp.float32)


def draw_activations(key, part):
    shared_key = jax.random.fold_in(key, 11)
    fresh_key = jax.random.fold_in(key, 23)
    shard_key = jax.random.fold_in(key, 41)
    column_key = jax.random.fold_in(key, 53)
    shared_part = jax.random.normal(shared_key, (TOKENS, 1, D), jnp.float32)
    fresh_part = jax.random.normal(fresh_key, (TOKENS, L, D), jnp.float32)
    token_scale = jnp.ones((TOKENS, 1, 1), jnp.float32)
    shard_scale = jnp.exp(jax.random.uniform(shard_key, (TOKENS // TOK_DEV, 1, 1, 1), jnp.float32, -0.7, 0.7))
    column_scale = jnp.exp(jax.random.uniform(column_key, (1, L, D), jnp.float32, -0.7, 0.7))
    mixture = 0.75 * shared_part + 0.66 * fresh_part
    mixture = mixture.reshape(TOKENS, L, NB, B)
    mixture = jnp.einsum('tlgi,ji->tlgj', mixture, column_filter(), precision=lax.Precision.HIGHEST)
    mixture = mixture.reshape(TOKENS, L, D) * token_scale * column_scale
    mixture = (mixture.reshape(TOKENS // TOK_DEV, TOK_DEV, L, D) * shard_scale).reshape(TOKENS, L, D)
    return jnp.clip(mixture, -8.0, 8.0).astype(jnp.bfloat16)


def block_levels(key, shape, cuts, least, high):
    gain, own = 1.0, jax.random.fold_in(key, 6)
    for position, shards_of in cuts:
        heights = jnp.exp(jax.random.uniform(jax.random.fold_in(own, position), (shards_of,), jnp.float32, least / len(cuts), high / len(cuts)))
        gain = gain * jnp.repeat(heights, shape[position] // shards_of).reshape([-1 if axis == position else 1 for axis in range(len(shape))])
    return gain


def setup_inputs(seed: int = 0) -> dict:
    key_of = jax.random.split(jax.random.key(seed), 3)
    activations = draw_activations(jax.random.fold_in(key_of[2], 71), 0)
    damping = jnp.clip(jnp.exp(math.log(1.0) - 2.3025851 * jax.random.uniform(key_of[1], (L,), jnp.float32) ** block_levels(key_of[1], (L,), ((0, 4),), -0.2, 0.2)), 0.1, 1.0)
    return dict(activations=activations, damping=damping)


def layer_grams(activations, index):
    current = lax.dynamic_index_in_dim(activations, index, 1, keepdims=False)
    current = current.astype(jnp.float32).reshape(TOKENS, NB, B)
    later = jnp.minimum(index + 1, L - 1).astype(jnp.int32)
    following = lax.dynamic_index_in_dim(activations, later, 1, keepdims=False)
    following = following.astype(jnp.float32).reshape(TOKENS, NB, B)
    diagonal = jnp.einsum('tgb,tgc->gbc', current, current, precision=lax.Precision.HIGHEST) / TOKENS
    crossed = jnp.einsum('tgb,tgc->gbc', current, following, precision=lax.Precision.HIGHEST) / TOKENS
    return (diagonal, crossed)

def solve_block(system, right_side):
    factor = jnp.linalg.cholesky(system)
    return jax.scipy.linalg.cho_solve((factor, True), right_side)

def reference(activations, damping):
    diagonal_gram, cross_gram = lax.map(partial(layer_grams, activations), jnp.arange(L, dtype=jnp.int32))
    trace_mean = jnp.sum(jnp.trace(diagonal_gram, axis1=2, axis2=3), axis=1) / D
    identity = jnp.eye(B, dtype=jnp.float32)
    damped = diagonal_gram + (damping * trace_mean)[:, None, None, None] * identity
    final_mask = (jnp.arange(L) == L - 1)[:, None, None, None]
    following = jnp.concatenate([damped[1:], damped[:1]], axis=0)
    following = jnp.where(final_mask, identity, following)
    cross_gram = jnp.where(final_mask, jnp.zeros_like(cross_gram), cross_gram)
    damped = damped.reshape(L * NB, B, B)
    following = following.reshape(L * NB, B, B)
    cross_gram = cross_gram.reshape(L * NB, B, B)
    coupling_t = jax.vmap(solve_block)(following, jnp.swapaxes(cross_gram, 1, 2))
    schur = damped - jnp.matmul(cross_gram, coupling_t, precision=lax.Precision.HIGHEST)
    identities = jnp.broadcast_to(identity, schur.shape)
    schur_inverse = jax.vmap(solve_block)(schur, identities)
    return (schur_inverse, jnp.swapaxes(coupling_t, 1, 2))
```

```python
import functools

import jax
import jax.numpy as jnp
from jax import lax
from jax.experimental import pallas as pl
from jax.experimental.pallas import tpu as pltpu
from jax.sharding import PartitionSpec as P

MESH = pl.DeviceIdType.MESH
HIGHEST = lax.Precision.HIGHEST
B = 128
W = 16
NY, NX, NZ = 4, 2, 8
PIECES = 4
PEERS = ((0, 1), (1, 0), (3, 0), (1, 1), (3, 1), (2, 0), (2, 1))
UNITS = ((0, 0), (1, 0), (0, 1), (2, 0), (1, 1), (3, 0), (2, 1), (3, 1))


def product(a, b):
    return lax.dot_general(
        a, b, (((1,), (0,)), ((), ())), precision=HIGHEST, preferred_element_type=jnp.float32
    )


def product_t(a, b):
    return lax.dot_general(
        a, b, (((1,), (1,)), ((), ())), precision=HIGHEST, preferred_element_type=jnp.float32
    )


def gram(a, b):
    return lax.dot_general(a, b, (((0,), (0,)), ((), ())), preferred_element_type=jnp.float32)


def small_inverse(panel, first):
    row = lax.broadcasted_iota(jnp.int32, (8, B), 0)
    halves = [panel[8 * h : 8 * h + 8] for h in range(W // 8)]
    columns = [
        [jnp.broadcast_to(half[:, first + j : first + j + 1], (8, B)) for half in halves]
        for j in range(W)
    ]
    for j in range(W):
        h, i = divmod(j, 8)
        own = row == i
        pivot = columns[j]
        inverse = 1.0 / pivot[h][i : i + 1]
        for k in range(W):
            if k == j:
                continue
            scaled = columns[k][h][i : i + 1] * inverse
            new = [c - p * scaled for c, p in zip(columns[k], pivot)]
            new[h] = jnp.where(own, scaled, new[h])
            columns[k] = new
        new = [-p * inverse for p in pivot]
        new[h] = jnp.where(own, inverse, new[h])
        columns[j] = new
    return columns


def invert(a):
    lane = lax.broadcasted_iota(jnp.int32, (B, B), 1)
    row = lax.broadcasted_iota(jnp.int32, (W, B), 0)
    for first in range(0, B, W):
        panel = a[first : first + W]
        columns = small_inverse(panel, first)
        inside = (lane >= first) & (lane < first + W)
        identity = (lane[:W] - first == row).astype(jnp.float32)
        rows = jnp.where(inside[:W], identity, panel)
        halves = []
        for h in range(W // 8):
            total = columns[0][h] * rows[0:1]
            for j in range(1, W):
                total = total + columns[j][h] * rows[j : j + 1]
            halves.append(total)
        rows = jnp.concatenate(halves, axis=0)
        rest = jnp.where(inside, 0.0, a) - product(a[:, first : first + W], rows)
        parts = [rest[:first]] if first else []
        parts.append(rows)
        if first + W < B:
            parts.append(rest[first + W :])
        a = jnp.concatenate(parts, axis=0)
    return a


def solve_kernel(diagonal_ref, cross_ref, following_ref, level_ref, inverse_ref, coupling_ref):
    diagonal = lax.broadcasted_iota(jnp.int32, (B, B), 0) == lax.broadcasted_iota(
        jnp.int32, (B, B), 1
    )
    cross = cross_ref[...]
    following = following_ref[...]
    following = jnp.where(diagonal, following + level_ref[1, 0:1, :], following)
    coupling = product(cross, invert(following))
    coupling_ref[0] = coupling
    damped = diagonal_ref[...]
    damped = jnp.where(diagonal, damped + level_ref[0, 0:1, :], damped)
    inverse_ref[0] = invert(damped - product_t(coupling, cross))


def filled(ref, semaphore):
    pltpu.make_async_copy(ref, ref, semaphore).wait()


def gram_kernel(
    tokens,
    x_ref,
    damping_ref,
    diagonal_ref,
    cross_ref,
    following_ref,
    level_ref,
    raw,
    passed,
    partial,
    got,
    reduced,
    follow,
    square,
    square_a,
    square_b,
    square_c,
    level,
    level_next,
    raw_send,
    raw_recv,
    pass_send,
    pass_recv,
    part_send,
    part_recv,
    follow_sem,
    square_send,
    square_recv,
    level_sem,
):
    section, dp = lax.axis_index("section"), lax.axis_index("dp")
    sections = lax.axis_size("section")
    y, x, z = dp // (NX * NZ), (dp // NZ) % NX, dp % NZ
    upper = y // 2
    has_before, has_after = section > 0, section < sections - 1
    before, after = lax.rem(section + sections - 1, sections), lax.rem(section + 1, sections)
    across = lax.rem(y + 2, NY)

    def at(y, x, z):
        return y * (NX * NZ) + x * NZ + z

    def near(dy, dx):
        return lax.rem(y + dy, NY), lax.rem(x + dx, NX)

    def send(src, dst, send_sem, recv_sem, to_section, to_dp):
        return pltpu.make_async_remote_copy(
            src_ref=src,
            dst_ref=dst,
            send_sem=send_sem,
            recv_sem=recv_sem,
            device_id=(to_section, to_dp),
            device_id_type=MESH,
        )

    barrier = pltpu.get_barrier_semaphore()
    greeted = [(section, at(*near(dy, dx), z)) for dy, dx in PEERS]
    for dz in range(1, NZ):
        other = lax.rem(z + dz, NZ)
        greeted += [(section, at(y, x, other)), (section, at(across, x, other))]
    greeted += [(before, dp), (after, dp)]
    greeted += [(jnp.where(upper == 0, before, after), at(across, x, z))]
    for device in greeted:
        pl.semaphore_signal(barrier, inc=1, device_id=device, device_id_type=MESH)
    pl.semaphore_wait(barrier, len(greeted))

    def order(piece):
        return lax.rem(piece + z // 2 + 1, PIECES)

    def source(piece, layer, y, x):
        block = lax.rem(y, 2) * (NX * NZ) + x * NZ + 2 * order(piece) + y // 2
        return x_ref.at[layer, :, pl.ds(pl.multiple_of(block * B, B), B)]

    def start(piece, layer):
        pltpu.make_async_copy(
            source(piece, layer, y, x), raw.at[piece, layer, 0], raw_recv.at[piece, layer]
        ).start()
        for slot, (dy, dx) in enumerate(PEERS, 1):
            to_y, to_x = near(dy, dx)
            send(
                source(piece, layer, to_y, to_x),
                raw.at[piece, layer, slot],
                raw_send,
                raw_recv.at[piece, layer],
                section,
                at(to_y, to_x, z),
            ).start()

    for piece, layer in UNITS[:2]:
        start(piece, layer)

    width = x_ref.shape[2]

    def add_rows(step, totals):
        rows = pl.ds(pl.multiple_of(step * 16, 16), 16)
        out = []
        for layer in range(2):
            total = totals[layer]
            for c in range(width // B):
                value = x_ref[layer, rows, c * B : (c + 1) * B].astype(jnp.float32)
                total = total + value * value
            out.append(total)
        return tuple(out)

    zero = jnp.zeros((16, B), jnp.float32)
    totals = lax.fori_loop(0, x_ref.shape[1] // 16, add_rows, (zero, zero))
    for layer in range(2):
        square[layer] = totals[layer][:8] + totals[layer][8:]
    for slot, (dy, dx) in enumerate(PEERS):
        to_y, to_x = near(dy, dx)
        send(
            square, square_a.at[slot], square_send.at[0], square_recv.at[0], section, at(to_y, to_x, z)
        ).start()
    for piece, layer in UNITS[2:]:
        start(piece, layer)
    filled(square_a, square_recv.at[0])
    total = square[...]
    for slot in range(len(PEERS)):
        total = total + square_a[slot]
    square_c[...] = total
    for dz in range(1, NZ):
        send(
            square_c,
            square_b.at[dz - 1],
            square_send.at[1],
            square_recv.at[1],
            section,
            at(y, x, lax.rem(z + dz, NZ)),
        ).start()

    def target(piece, layer):
        to_y, to_z = lax.rem(y, 2) + 2 * layer, 2 * order(piece) + upper
        return at(to_y, x, to_z), (to_y == y) & (to_z == z)

    def item(piece, layer):
        to_dp, own = target(piece, layer)
        src, dst = partial.at[piece, layer], got.at[z]
        remote = send(src, dst, part_send.at[piece, layer], part_recv, section, to_dp)
        local = pltpu.make_async_copy(src, dst, part_recv)
        return remote, local, own

    def deliver(piece, layer):
        remote, local, own = item(piece, layer)

        @pl.when(own)
        def _():
            local.start()

        @pl.when(jnp.logical_not(own))
        def _():
            remote.start()

    def passing(piece):
        return send(
            raw.at[piece, 0], passed.at[piece], pass_send.at[piece], pass_recv.at[piece], before, dp
        )

    depth = len(PEERS) + 1

    def columns(ref):
        return ref[...].reshape(depth * x_ref.shape[1], B)

    for unit, (piece, layer) in enumerate(UNITS):
        filled(raw.at[piece, layer], raw_recv.at[piece, layer])
        if layer == 0:

            @pl.when(has_before)
            def _():
                passing(piece).start()

        else:
            first, second = columns(raw.at[piece, 0]), columns(raw.at[piece, 1])
            partial[piece, 0, 0] = gram(first, first)
            partial[piece, 0, 1] = gram(first, second)
            deliver(piece, 0)
            partial[piece, 1, 0] = gram(second, second)

            @pl.when(has_after)
            def _():
                filled(passed.at[piece], pass_recv.at[piece])
                partial[piece, 1, 1] = gram(second, columns(passed.at[piece]))

            @pl.when(jnp.logical_not(has_after))
            def _():
                partial[piece, 1, 1] = jnp.zeros((B, B), jnp.float32)

            deliver(piece, 1)
        if unit == 2:
            filled(square_b, square_recv.at[1])
            total = square_c[...]
            for dz in range(1, NZ):
                total = total + square_b[dz - 1]
            for own_layer in range(2):
                trace = jnp.sum(total[own_layer], keepdims=True) * (1.0 / (tokens * width))
                level[own_layer] = jnp.broadcast_to(trace, (8, B)) * damping_ref[own_layer]

            @pl.when(has_before)
            def _():
                send(
                    level.at[0], level_next, level_sem.at[0], level_sem.at[1], before, dp
                ).start()

    filled(got, part_recv)
    for which, out in enumerate((reduced, cross_ref)):
        total = got[0, which]
        for step in range(1, NZ):
            total = total + got[step, which]
        out[...] = total * (1.0 / tokens)
    follows = send(
        reduced,
        follow,
        follow_sem.at[0],
        follow_sem.at[1],
        jnp.where(upper == 0, before, section),
        at(across, x, z),
    )
    first_of_all = jnp.logical_not(has_before) & (upper == 0)
    last_of_all = jnp.logical_not(has_after) & (upper == 1)

    @pl.when(jnp.logical_not(first_of_all))
    def _():
        follows.start()

    diagonal_ref[...] = reduced[...]

    @pl.when(has_after)
    def _():
        filled(level_next, level_sem.at[1])

    @pl.when(upper == 0)
    def _():
        level_ref[0] = level[0]
        level_ref[1] = level[1]

    @pl.when((upper == 1) & has_after)
    def _():
        level_ref[0] = level[1]
        level_ref[1] = level_next[...]

    @pl.when(last_of_all)
    def _():
        level_ref[0] = level[1]
        level_ref[1] = jnp.zeros((8, B), jnp.float32)

    for piece in range(PIECES):
        for layer in range(2):
            remote, _, own = item(piece, layer)
            pl.when(jnp.logical_not(own))(remote.wait_send)
        pl.when(has_before)(passing(piece).wait_send)
    sent = raw.at[:, :, pl.ds(1, len(PEERS))]
    filled(sent, raw_send)
    filled(square_a, square_send.at[0])
    filled(square_b, square_send.at[1])

    @pl.when(has_before)
    def _():
        filled(level_next, level_sem.at[0])

    @pl.when(last_of_all)
    def _():
        following_ref[...] = (
            lax.broadcasted_iota(jnp.int32, (B, B), 0) == lax.broadcasted_iota(jnp.int32, (B, B), 1)
        ).astype(jnp.float32)
        cross_ref[...] = jnp.zeros((B, B), jnp.float32)

    @pl.when(jnp.logical_not(last_of_all))
    def _():
        filled(follow, follow_sem.at[1])
        following_ref[...] = follow[...]

    @pl.when(jnp.logical_not(first_of_all))
    def _():
        filled(follow, follow_sem.at[0])


def local(activations, damping):
    rows, layers, width = activations.shape
    tokens = rows * lax.axis_size("dp")
    by_layer = jnp.transpose(activations, (1, 0, 2))
    depth = len(PEERS) + 1
    f32, bf16 = jnp.float32, jnp.bfloat16
    vmem = pl.BlockSpec(memory_space=pltpu.VMEM)
    block = jax.ShapeDtypeStruct((B, B), f32)
    diagonal, cross, following, level = pl.pallas_call(
        functools.partial(gram_kernel, tokens),
        out_shape=(block, block, block, jax.ShapeDtypeStruct((2, 8, B), f32)),
        in_specs=[vmem, pl.BlockSpec(memory_space=pltpu.SMEM)],
        out_specs=(vmem,) * 4,
        scratch_shapes=[
            pltpu.VMEM((PIECES, 2, depth, rows, B), bf16),
            pltpu.VMEM((PIECES, depth, rows, B), bf16),
            pltpu.VMEM((PIECES, 2, 2, B, B), f32),
            pltpu.VMEM((NZ, 2, B, B), f32),
            pltpu.VMEM((B, B), f32),
            pltpu.VMEM((B, B), f32),
            pltpu.VMEM((2, 8, B), f32),
            pltpu.VMEM((len(PEERS), 2, 8, B), f32),
            pltpu.VMEM((NZ - 1, 2, 8, B), f32),
            pltpu.VMEM((2, 8, B), f32),
            pltpu.VMEM((2, 8, B), f32),
            pltpu.VMEM((8, B), f32),
            pltpu.SemaphoreType.DMA,
            pltpu.SemaphoreType.DMA((PIECES, 2)),
            pltpu.SemaphoreType.DMA((PIECES,)),
            pltpu.SemaphoreType.DMA((PIECES,)),
            pltpu.SemaphoreType.DMA((PIECES, 2)),
            pltpu.SemaphoreType.DMA,
            pltpu.SemaphoreType.DMA((2,)),
            pltpu.SemaphoreType.DMA((2,)),
            pltpu.SemaphoreType.DMA((2,)),
            pltpu.SemaphoreType.DMA((2,)),
        ],
        compiler_params=pltpu.CompilerParams(
            collective_id=0, has_side_effects=True, vmem_limit_bytes=32 * 2**20
        ),
        name="grams",
    )(by_layer, damping)
    result = jax.ShapeDtypeStruct((1, B, B), f32)
    return pl.pallas_call(solve_kernel, out_shape=(result, result), name="solve")(
        diagonal, cross, following, level
    )


def solution(mesh):
    placed = (P("dp", "section", None), P("section"))
    return jax.shard_map(
        local,
        mesh=mesh,
        in_specs=placed,
        out_specs=(P(("section", "dp"), None, None), P(("section", "dp"), None, None)),
        check_vma=False,
    )
```

```python
import functools

import jax
import jax.numpy as jnp
from jax import lax
from jax.experimental import pallas as pl
from jax.experimental.pallas import tpu as pltpu
from jax.sharding import PartitionSpec as P

MESH = pl.DeviceIdType.MESH
HIGHEST = lax.Precision.HIGHEST
B = 128
W = 16
NY, NX, NZ = 4, 2, 8
PIECES = 4
PEERS = ((0, 1), (1, 0), (3, 0), (1, 1), (3, 1), (2, 0), (2, 1))
AHEAD = 4
UNITS = ((0, 0), (1, 0), (0, 1), (2, 0), (1, 1), (3, 0), (2, 1), (3, 1))


def product(a, b):
    return lax.dot_general(
        a, b, (((1,), (0,)), ((), ())), precision=HIGHEST, preferred_element_type=jnp.float32
    )


def product_t(a, b):
    return lax.dot_general(
        a, b, (((1,), (1,)), ((), ())), precision=HIGHEST, preferred_element_type=jnp.float32
    )


def gram(a, b):
    return lax.dot_general(a, b, (((0,), (0,)), ((), ())), preferred_element_type=jnp.float32)


def small_inverse(panel, first):
    row = lax.broadcasted_iota(jnp.int32, (8, B), 0)
    halves = [panel[8 * h : 8 * h + 8] for h in range(W // 8)]
    columns = [
        [jnp.broadcast_to(half[:, first + j : first + j + 1], (8, B)) for half in halves]
        for j in range(W)
    ]
    for j in range(W):
        h, i = divmod(j, 8)
        own = row == i
        pivot = columns[j]
        inverse = 1.0 / pivot[h][i : i + 1]
        for k in range(W):
            if k == j:
                continue
            scaled = columns[k][h][i : i + 1] * inverse
            new = [c - p * scaled for c, p in zip(columns[k], pivot)]
            new[h] = jnp.where(own, scaled, new[h])
            columns[k] = new
        new = [-p * inverse for p in pivot]
        new[h] = jnp.where(own, inverse, new[h])
        columns[j] = new
    return columns


def invert(a):
    lane = lax.broadcasted_iota(jnp.int32, (B, B), 1)
    row = lax.broadcasted_iota(jnp.int32, (W, B), 0)
    for first in range(0, B, W):
        panel = a[first : first + W]
        columns = small_inverse(panel, first)
        inside = (lane >= first) & (lane < first + W)
        identity = (lane[:W] - first == row).astype(jnp.float32)
        rows = jnp.where(inside[:W], identity, panel)
        halves = []
        for h in range(W // 8):
            total = columns[0][h] * rows[0:1]
            for j in range(1, W):
                total = total + columns[j][h] * rows[j : j + 1]
            halves.append(total)
        rows = jnp.concatenate(halves, axis=0)
        rest = jnp.where(inside, 0.0, a) - product(a[:, first : first + W], rows)
        parts = [rest[:first]] if first else []
        parts.append(rows)
        if first + W < B:
            parts.append(rest[first + W :])
        a = jnp.concatenate(parts, axis=0)
    return a


def solve_kernel(diagonal_ref, cross_ref, following_ref, level_ref, inverse_ref, coupling_ref):
    diagonal = lax.broadcasted_iota(jnp.int32, (B, B), 0) == lax.broadcasted_iota(
        jnp.int32, (B, B), 1
    )
    cross = cross_ref[...]
    following = following_ref[...]
    following = jnp.where(diagonal, following + level_ref[1, 0:1, :], following)
    coupling = product(cross, invert(following))
    coupling_ref[0] = coupling
    damped = diagonal_ref[...]
    damped = jnp.where(diagonal, damped + level_ref[0, 0:1, :], damped)
    inverse_ref[0] = invert(damped - product_t(coupling, cross))


def filled(ref, semaphore):
    pltpu.make_async_copy(ref, ref, semaphore).wait()


def gram_kernel(
    tokens,
    x_ref,
    damping_ref,
    diagonal_ref,
    cross_ref,
    following_ref,
    level_ref,
    raw,
    passed,
    partial,
    got,
    reduced,
    moved,
    follow,
    square,
    square_a,
    square_b,
    square_c,
    level,
    level_next,
    raw_send,
    raw_recv,
    pass_send,
    pass_recv,
    part_send,
    part_recv,
    move_sem,
    follow_sem,
    square_send,
    square_recv,
    level_sem,
):
    section, dp = lax.axis_index("section"), lax.axis_index("dp")
    sections = lax.axis_size("section")
    y, x, z = dp // (NX * NZ), (dp // NZ) % NX, dp % NZ
    upper = y // 2
    has_before, has_after = section > 0, section < sections - 1
    before, after = lax.rem(section + sections - 1, sections), lax.rem(section + 1, sections)
    across = lax.rem(y + 2, NY)
    beside = z + 1 - 2 * lax.rem(z, 2)
    keeps = lax.rem(z, 2) == upper

    def at(y, x, z):
        return y * (NX * NZ) + x * NZ + z

    def near(dy, dx):
        return lax.rem(y + dy, NY), lax.rem(x + dx, NX)

    def send(src, dst, send_sem, recv_sem, to_section, to_dp):
        return pltpu.make_async_remote_copy(
            src_ref=src,
            dst_ref=dst,
            send_sem=send_sem,
            recv_sem=recv_sem,
            device_id=(to_section, to_dp),
            device_id_type=MESH,
        )

    barrier = pltpu.get_barrier_semaphore()
    greeted = [(section, at(*near(dy, dx), z)) for dy, dx in PEERS]
    for dz in range(1, NZ):
        other = lax.rem(z + dz, NZ)
        greeted += [(section, at(y, x, other))]
    greeted += [(before, dp), (after, dp), (section, at(across, x, beside))]
    greeted += [(before, at(other_y, x, other_z)) for other_y, other_z in ((across, z), (y, beside))]
    greeted += [(after, at(other_y, x, other_z)) for other_y, other_z in ((across, z), (y, beside))]
    for device in greeted:
        pl.semaphore_signal(barrier, inc=1, device_id=device, device_id_type=MESH)
    pl.semaphore_wait(barrier, len(greeted))

    def order(piece):
        return lax.rem(piece + z // 2 + 1, PIECES)

    def source(piece, layer, y, x):
        block = lax.rem(y, 2) * (NX * NZ) + x * NZ + 2 * order(piece) + y // 2
        return x_ref.at[layer, :, pl.ds(pl.multiple_of(block * B, B), B)]

    def start(piece, layer):
        pltpu.make_async_copy(
            source(piece, layer, y, x), raw.at[piece, layer, 0], raw_recv.at[piece, layer]
        ).start()
        for slot, (dy, dx) in enumerate(PEERS, 1):
            to_y, to_x = near(dy, dx)
            send(
                source(piece, layer, to_y, to_x),
                raw.at[piece, layer, slot],
                raw_send,
                raw_recv.at[piece, layer],
                section,
                at(to_y, to_x, z),
            ).start()

    for piece, layer in UNITS[:2]:
        start(piece, layer)

    width = x_ref.shape[2]

    def add_rows(step, totals):
        rows = pl.ds(pl.multiple_of(step * 16, 16), 16)
        out = []
        for layer in range(2):
            total = totals[layer]
            for c in range(width // B):
                value = x_ref[layer, rows, c * B : (c + 1) * B].astype(jnp.float32)
                total = total + value * value
            out.append(total)
        return tuple(out)

    zero = jnp.zeros((16, B), jnp.float32)
    totals = lax.fori_loop(0, x_ref.shape[1] // 16, add_rows, (zero, zero))
    for layer in range(2):
        square[layer] = totals[layer][:8] + totals[layer][8:]
    for slot, (dy, dx) in enumerate(PEERS):
        to_y, to_x = near(dy, dx)
        send(
            square, square_a.at[slot], square_send.at[0], square_recv.at[0], section, at(to_y, to_x, z)
        ).start()
    for piece, layer in UNITS[2:AHEAD]:
        start(piece, layer)
    filled(square_a, square_recv.at[0])
    total = square[...]
    for slot in range(len(PEERS)):
        total = total + square_a[slot]
    square_c[...] = total
    for dz in range(1, NZ):
        send(
            square_c,
            square_b.at[dz - 1],
            square_send.at[1],
            square_recv.at[1],
            section,
            at(y, x, lax.rem(z + dz, NZ)),
        ).start()

    def target(piece, layer):
        to_z = 2 * order(piece) + layer
        return at(y, x, to_z), to_z == z

    def item(piece, layer):
        to_dp, own = target(piece, layer)
        src, dst = partial.at[piece, layer], got.at[z]
        remote = send(src, dst, part_send.at[piece, layer], part_recv, section, to_dp)
        local = pltpu.make_async_copy(src, dst, part_recv)
        return remote, local, own

    def deliver(piece, layer):
        remote, local, own = item(piece, layer)

        @pl.when(own)
        def _():
            local.start()

        @pl.when(jnp.logical_not(own))
        def _():
            remote.start()

    def passing(piece):
        return send(
            raw.at[piece, 0], passed.at[piece], pass_send.at[piece], pass_recv.at[piece], before, dp
        )

    depth = len(PEERS) + 1

    def columns(ref):
        return ref[...].reshape(depth * x_ref.shape[1], B)

    for unit, (piece, layer) in enumerate(UNITS):
        filled(raw.at[piece, layer], raw_recv.at[piece, layer])
        if layer == 0:

            @pl.when(has_before)
            def _():
                passing(piece).start()

        else:
            first, second = columns(raw.at[piece, 0]), columns(raw.at[piece, 1])
            partial[piece, 0, 0] = gram(first, first)
            partial[piece, 0, 1] = gram(first, second)
            deliver(piece, 0)
            partial[piece, 1, 0] = gram(second, second)

            @pl.when(has_after)
            def _():
                filled(passed.at[piece], pass_recv.at[piece])
                partial[piece, 1, 1] = gram(second, columns(passed.at[piece]))

            @pl.when(jnp.logical_not(has_after))
            def _():
                partial[piece, 1, 1] = jnp.zeros((B, B), jnp.float32)

            deliver(piece, 1)
        if unit + AHEAD < len(UNITS):
            start(*UNITS[unit + AHEAD])
        if unit == 2:
            filled(square_b, square_recv.at[1])
            total = square_c[...]
            for dz in range(1, NZ):
                total = total + square_b[dz - 1]
            for own_layer in range(2):
                trace = jnp.sum(total[own_layer], keepdims=True) * (1.0 / (tokens * width))
                level[own_layer] = jnp.broadcast_to(trace, (8, B)) * damping_ref[own_layer]

            @pl.when(has_before)
            def _():
                send(
                    level.at[0], level_next, level_sem.at[0], level_sem.at[1], before, dp
                ).start()

    filled(got, part_recv)
    for which in range(2):
        total = got[0, which]
        for step in range(1, NZ):
            total = total + got[step, which]
        reduced[which] = total * (1.0 / tokens)
    layer_here = jnp.where(keeps, upper, 1 - upper)
    moves = send(
        reduced, moved, move_sem.at[0], move_sem.at[1], section, at(across, x, beside)
    )
    follows = send(
        reduced.at[0],
        follow,
        follow_sem.at[0],
        follow_sem.at[1],
        jnp.where(layer_here == 0, before, section),
        at(jnp.where(keeps, across, y), x, jnp.where(keeps, z, beside)),
    )
    first_of_all = jnp.logical_not(has_before) & (layer_here == 0)
    last_of_all = jnp.logical_not(has_after) & (upper == 1)

    @pl.when(jnp.logical_not(first_of_all))
    def _():
        follows.start()

    @pl.when(jnp.logical_not(keeps))
    def _():
        moves.start()

    @pl.when(has_after)
    def _():
        filled(level_next, level_sem.at[1])

    @pl.when(upper == 0)
    def _():
        level_ref[0] = level[0]
        level_ref[1] = level[1]

    @pl.when((upper == 1) & has_after)
    def _():
        level_ref[0] = level[1]
        level_ref[1] = level_next[...]

    @pl.when(last_of_all)
    def _():
        level_ref[0] = level[1]
        level_ref[1] = jnp.zeros((8, B), jnp.float32)

    for piece in range(PIECES):
        for layer in range(2):
            remote, _, own = item(piece, layer)
            pl.when(jnp.logical_not(own))(remote.wait_send)
        pl.when(has_before)(passing(piece).wait_send)
    sent = raw.at[:, :, pl.ds(1, len(PEERS))]
    filled(sent, raw_send)
    filled(square_a, square_send.at[0])
    filled(square_b, square_send.at[1])

    @pl.when(has_before)
    def _():
        filled(level_next, level_sem.at[0])

    @pl.when(keeps)
    def _():
        diagonal_ref[...] = reduced[0]
        cross_ref[...] = reduced[1]

    @pl.when(jnp.logical_not(keeps))
    def _():
        filled(moved, move_sem.at[1])
        diagonal_ref[...] = moved[0]
        cross_ref[...] = moved[1]

    @pl.when(last_of_all)
    def _():
        following_ref[...] = (
            lax.broadcasted_iota(jnp.int32, (B, B), 0) == lax.broadcasted_iota(jnp.int32, (B, B), 1)
        ).astype(jnp.float32)
        cross_ref[...] = jnp.zeros((B, B), jnp.float32)

    @pl.when(jnp.logical_not(last_of_all))
    def _():
        filled(follow, follow_sem.at[1])
        following_ref[...] = follow[...]

    @pl.when(jnp.logical_not(keeps))
    def _():
        filled(moved, move_sem.at[0])

    @pl.when(jnp.logical_not(first_of_all))
    def _():
        filled(follow, follow_sem.at[0])


def local(activations, damping):
    rows, layers, width = activations.shape
    tokens = rows * lax.axis_size("dp")
    by_layer = jnp.transpose(activations, (1, 0, 2))
    depth = len(PEERS) + 1
    f32, bf16 = jnp.float32, jnp.bfloat16
    vmem = pl.BlockSpec(memory_space=pltpu.VMEM)
    block = jax.ShapeDtypeStruct((B, B), f32)
    diagonal, cross, following, level = pl.pallas_call(
        functools.partial(gram_kernel, tokens),
        out_shape=(block, block, block, jax.ShapeDtypeStruct((2, 8, B), f32)),
        in_specs=[vmem, pl.BlockSpec(memory_space=pltpu.SMEM)],
        out_specs=(vmem,) * 4,
        scratch_shapes=[
            pltpu.VMEM((PIECES, 2, depth, rows, B), bf16),
            pltpu.VMEM((PIECES, depth, rows, B), bf16),
            pltpu.VMEM((PIECES, 2, 2, B, B), f32),
            pltpu.VMEM((NZ, 2, B, B), f32),
            pltpu.VMEM((2, B, B), f32),
            pltpu.VMEM((2, B, B), f32),
            pltpu.VMEM((B, B), f32),
            pltpu.VMEM((2, 8, B), f32),
            pltpu.VMEM((len(PEERS), 2, 8, B), f32),
            pltpu.VMEM((NZ - 1, 2, 8, B), f32),
            pltpu.VMEM((2, 8, B), f32),
            pltpu.VMEM((2, 8, B), f32),
            pltpu.VMEM((8, B), f32),
            pltpu.SemaphoreType.DMA,
            pltpu.SemaphoreType.DMA((PIECES, 2)),
            pltpu.SemaphoreType.DMA((PIECES,)),
            pltpu.SemaphoreType.DMA((PIECES,)),
            pltpu.SemaphoreType.DMA((PIECES, 2)),
            pltpu.SemaphoreType.DMA,
            pltpu.SemaphoreType.DMA((2,)),
            pltpu.SemaphoreType.DMA((2,)),
            pltpu.SemaphoreType.DMA((2,)),
            pltpu.SemaphoreType.DMA((2,)),
            pltpu.SemaphoreType.DMA((2,)),
        ],
        compiler_params=pltpu.CompilerParams(
            collective_id=0, has_side_effects=True, vmem_limit_bytes=32 * 2**20
        ),
        name="grams",
    )(by_layer, damping)
    result = jax.ShapeDtypeStruct((1, B, B), f32)
    return pl.pallas_call(
        solve_kernel,
        out_shape=(result, result),
        in_specs=[vmem] * 4,
        compiler_params=pltpu.CompilerParams(vmem_limit_bytes=8 * 2**20),
        name="solve",
    )(diagonal, cross, following, level)


def solution(mesh):
    placed = (P("dp", "section", None), P("section"))
    return jax.shard_map(
        local,
        mesh=mesh,
        in_specs=placed,
        out_specs=(P(("section", "dp"), None, None), P(("section", "dp"), None, None)),
        check_vma=False,
    )
```

```python
import functools

import jax
import jax.numpy as jnp
from jax import lax
from jax.experimental import pallas as pl
from jax.experimental.pallas import tpu as pltpu
from jax.sharding import PartitionSpec as P

MESH = pl.DeviceIdType.MESH
HIGHEST = lax.Precision.HIGHEST
B = 128
W = 16
NY, NX, NZ = 4, 2, 8
PIECES = 4
PEERS = ((0, 1), (1, 0), (3, 0), (1, 1), (3, 1), (2, 0), (2, 1))
TURN = (2, 1, 3, 0)
LENT = (0, 2)
LATER = 3
AHEAD = 4
UNITS = tuple((piece, layer) for piece in range(PIECES) for layer in range(2))


def product(a, b):
    return lax.dot_general(
        a, b, (((1,), (0,)), ((), ())), precision=HIGHEST, preferred_element_type=jnp.float32
    )


def product_t(a, b):
    return lax.dot_general(
        a, b, (((1,), (1,)), ((), ())), precision=HIGHEST, preferred_element_type=jnp.float32
    )


def gram(a, b):
    return lax.dot_general(a, b, (((0,), (0,)), ((), ())), preferred_element_type=jnp.float32)


def small_inverse(panel, first):
    row = lax.broadcasted_iota(jnp.int32, (8, B), 0)
    halves = [panel[8 * h : 8 * h + 8] for h in range(W // 8)]
    columns = [
        [jnp.broadcast_to(half[:, first + j : first + j + 1], (8, B)) for half in halves]
        for j in range(W)
    ]
    for j in range(W):
        h, i = divmod(j, 8)
        own = row == i
        pivot = columns[j]
        inverse = 1.0 / pivot[h][i : i + 1]
        for k in range(W):
            if k == j:
                continue
            scaled = columns[k][h][i : i + 1] * inverse
            new = [c - p * scaled for c, p in zip(columns[k], pivot)]
            new[h] = jnp.where(own, scaled, new[h])
            columns[k] = new
        new = [-p * inverse for p in pivot]
        new[h] = jnp.where(own, inverse, new[h])
        columns[j] = new
    return columns


def invert(a):
    lane = lax.broadcasted_iota(jnp.int32, (B, B), 1)
    row = lax.broadcasted_iota(jnp.int32, (W, B), 0)
    panel = a[:W]
    for first in range(0, B, W):
        last = first + W
        columns = small_inverse(panel, first)
        inside = (lane >= first) & (lane < last)
        identity = (lane[:W] - first == row).astype(jnp.float32)
        panel = jnp.where(inside[:W], identity, panel)
        halves = []
        for h in range(W // 8):
            total = columns[0][h] * panel[0:1]
            for j in range(1, W):
                total = total + columns[j][h] * panel[j : j + 1]
            halves.append(total)
        rows = jnp.concatenate(halves, axis=0)
        halves = []
        for h in range(W // 8 if last < B else 0):
            below = a[last + 8 * h : last + 8 * h + 8]
            total = jnp.where(inside[:8], 0.0, below)
            for j in range(W):
                factor = jnp.broadcast_to(below[:, first + j : first + j + 1], (8, B))
                total = total - factor * rows[j : j + 1]
            halves.append(total)
        if halves:
            panel = jnp.concatenate(halves, axis=0)
        rest = jnp.where(inside, 0.0, a) - product(a[:, first:last], rows)
        parts = [rest[:first]] if first else []
        parts.append(rows)
        if last < B:
            parts.append(rest[last:])
        a = jnp.concatenate(parts, axis=0)
    return a


def solve_kernel(diagonal_ref, cross_ref, following_ref, level_ref, inverse_ref, coupling_ref):
    diagonal = lax.broadcasted_iota(jnp.int32, (B, B), 0) == lax.broadcasted_iota(
        jnp.int32, (B, B), 1
    )
    cross = cross_ref[...]
    following = following_ref[...]
    following = jnp.where(diagonal, following + level_ref[1, 0:1, :], following)
    coupling = product(cross, invert(following))
    coupling_ref[0] = coupling
    damped = diagonal_ref[...]
    damped = jnp.where(diagonal, damped + level_ref[0, 0:1, :], damped)
    inverse_ref[0] = invert(damped - product_t(coupling, cross))


def filled(ref, semaphore):
    pltpu.make_async_copy(ref, ref, semaphore).wait()


def gram_kernel(
    tokens,
    x_hbm,
    damping_ref,
    diagonal_ref,
    cross_ref,
    following_ref,
    level_ref,
    mixed,
    x_ref,
    raw,
    passed,
    lent,
    partial,
    returned,
    got,
    reduced,
    moved,
    follow,
    square,
    square_a,
    square_b,
    square_c,
    level,
    level_next,
    load_sem,
    raw_send,
    raw_recv,
    pass_send,
    pass_recv,
    lend_send,
    lend_recv,
    return_send,
    part_send,
    part_recv,
    move_sem,
    follow_sem,
    square_send,
    square_recv,
    level_sem,
):
    section, dp = lax.axis_index("section"), lax.axis_index("dp")
    sections = lax.axis_size("section")
    y, x, z = dp // (NX * NZ), (dp // NZ) % NX, dp % NZ
    upper = y // 2
    has_before, has_after = section > 0, section < sections - 1
    lends, borrows = section == sections // 2 - 1, section == sections // 2
    before, after = lax.rem(section + sections - 1, sections), lax.rem(section + 1, sections)
    across = lax.rem(y + 2, NY)
    beside = z + 1 - 2 * lax.rem(z, 2)
    keeps = lax.rem(z, 2) == upper

    def at(y, x, z):
        return y * (NX * NZ) + x * NZ + z

    def near(dy, dx):
        return lax.rem(y + dy, NY), lax.rem(x + dx, NX)

    def send(src, dst, send_sem, recv_sem, to_section, to_dp):
        return pltpu.make_async_remote_copy(
            src_ref=src,
            dst_ref=dst,
            send_sem=send_sem,
            recv_sem=recv_sem,
            device_id=(to_section, to_dp),
            device_id_type=MESH,
        )

    load = pltpu.make_async_copy(x_hbm, mixed, load_sem)
    load.start()
    barrier = pltpu.get_barrier_semaphore()
    greeted = [(section, at(*near(dy, dx), z)) for dy, dx in PEERS]
    for dz in range(1, NZ):
        other = lax.rem(z + dz, NZ)
        greeted += [(to_section, at(y, x, other)) for to_section in (before, section, after)]
    greeted += [(before, dp), (after, dp), (section, at(across, x, beside))]
    greeted += [(before, at(across, x, z)), (after, at(across, x, z))]
    for device in greeted:
        pl.semaphore_signal(barrier, inc=1, device_id=device, device_id_type=MESH)
    def order(piece):
        return lax.rem(z // 2 + TURN[piece], PIECES)

    def block_of(piece, y, x):
        return (y % 2) * (NX * NZ) + x * NZ + y // 2 + 2 * order(piece)

    def source(piece, layer, y, x):
        return x_ref.at[layer, block_of(piece, y, x)]

    rows, layers, width = mixed.shape
    part = rows // 2
    picked = lax.broadcasted_iota(jnp.int32, (layers * part, layers * part), 0)
    place = lax.broadcasted_iota(jnp.int32, (layers * part, layers * part), 1)
    picked = layers * (picked % part) + picked // part == place
    picked = picked.astype(jnp.bfloat16)

    def by_layer(piece):
        blocks = [block_of(piece, y, x) for y in range(NY) for x in range(NX)]
        for top in range(0, rows, part):
            both = jnp.concatenate(
                [
                    mixed[top : top + part, :, pl.ds(pl.multiple_of(block * B, B), B)]
                    for block in blocks
                ],
                axis=2,
            ).reshape(layers * part, len(blocks) * B)
            apart = lax.dot_general(
                picked, both, (((1,), (0,)), ((), ())), preferred_element_type=jnp.float32
            ).astype(jnp.bfloat16)
            for layer in range(layers):
                for i, block in enumerate(blocks):
                    x_ref[layer, block, top : top + part, :] = apart[
                        layer * part : (layer + 1) * part, i * B : (i + 1) * B
                    ]

    def start(piece, layer):
        pltpu.make_async_copy(
            source(piece, layer, y, x), raw.at[piece, layer, 0], raw_recv.at[piece, layer]
        ).start()
        for slot, (dy, dx) in enumerate(PEERS, 1):
            to_y, to_x = near(dy, dx)
            send(
                source(piece, layer, to_y, to_x),
                raw.at[piece, layer, slot],
                raw_send,
                raw_recv.at[piece, layer],
                section,
                at(to_y, to_x, z),
            ).start()

    load.wait()
    by_layer(0)
    pl.semaphore_wait(barrier, len(greeted))
    start(*UNITS[0])
    by_layer(1)
    start(*UNITS[1])
    start(*UNITS[2])
    by_layer(2)
    by_layer(3)

    def add_block(block, totals):
        out = []
        for layer in range(2):
            total = totals[layer]
            for top in range(0, rows, 16):
                value = x_ref[layer, block, top : top + 16, :].astype(jnp.float32)
                total = total + value * value
            out.append(total)
        return tuple(out)

    zero = jnp.zeros((16, B), jnp.float32)
    totals = lax.fori_loop(0, width // B, add_block, (zero, zero))
    for layer in range(2):
        square[layer] = totals[layer][:8] + totals[layer][8:]
    for slot, (dy, dx) in enumerate(PEERS):
        to_y, to_x = near(dy, dx)
        send(
            square, square_a.at[slot], square_send.at[0], square_recv.at[0], section, at(to_y, to_x, z)
        ).start()
    for piece, layer in UNITS[3:AHEAD]:
        start(piece, layer)
    filled(square_a, square_recv.at[0])
    total = square[...]
    for slot in range(len(PEERS)):
        total = total + square_a[slot]
    square_c[...] = total
    for dz in range(1, NZ):
        send(
            square_c,
            square_b.at[dz - 1],
            square_send.at[1],
            square_recv.at[1],
            section,
            at(y, x, lax.rem(z + dz, NZ)),
        ).start()

    def target(piece, layer):
        to_z = 2 * order(piece) + layer
        return at(y, x, to_z), to_z == z

    def item(piece, layer, which):
        to_dp, own = target(piece, layer)
        src, dst = partial.at[piece, layer, which], got.at[z, which]
        remote = send(src, dst, part_send.at[piece, layer, which], part_recv, section, to_dp)
        local = pltpu.make_async_copy(src, dst, part_recv)
        return remote, local, own

    def deliver(piece, layer, which):
        remote, local, own = item(piece, layer, which)

        @pl.when(own)
        def _():
            local.start()

        @pl.when(jnp.logical_not(own))
        def _():
            remote.start()

    def passing(piece):
        return send(
            raw.at[piece, 0], passed.at[piece], pass_send.at[piece], pass_recv.at[piece], before, dp
        )

    def lending(piece):
        slot = LENT.index(piece)
        return send(
            raw.at[piece, 1], lent.at[slot], lend_send.at[slot], lend_recv.at[slot], after, dp
        )

    def returning(piece):
        slot = LENT.index(piece)
        return send(
            returned.at[slot],
            got.at[z, 1],
            return_send.at[slot],
            part_recv,
            before,
            target(piece, 1)[0],
        )

    def passes(piece):
        return has_before & jnp.logical_not(borrows) if piece in LENT else has_before

    def receives(piece):
        return has_after & jnp.logical_not(lends) if piece in LENT else has_after

    depth = len(PEERS) + 1

    def columns(ref):
        return ref[...].reshape(depth * rows, B)

    for unit, (piece, layer) in enumerate(UNITS):
        filled(raw.at[piece, layer], raw_recv.at[piece, layer])
        if layer == 0:
            pl.when(passes(piece))(passing(piece).start)
        else:
            if piece in LENT:
                pl.when(lends)(lending(piece).start)
            first, second = columns(raw.at[piece, 0]), columns(raw.at[piece, 1])
            partial[piece, 0, 0] = gram(first, first)
            deliver(piece, 0, 0)
            partial[piece, 0, 1] = gram(first, second)
            deliver(piece, 0, 1)
            partial[piece, 1, 0] = gram(second, second)
            deliver(piece, 1, 0)

            @pl.when(receives(piece))
            def _():
                filled(passed.at[piece], pass_recv.at[piece])
                partial[piece, 1, 1] = gram(second, columns(passed.at[piece]))
                deliver(piece, 1, 1)

            @pl.when(jnp.logical_not(has_after))
            def _():
                partial[piece, 1, 1] = jnp.zeros((B, B), jnp.float32)
                deliver(piece, 1, 1)

        for slot, borrowed in enumerate(LENT):
            if unit == 2 * borrowed + LATER:

                @pl.when(borrows)
                def _():
                    filled(lent.at[slot], lend_recv.at[slot])
                    returned[slot] = gram(columns(lent.at[slot]), columns(raw.at[borrowed, 0]))
                    returning(borrowed).start()

        if unit + AHEAD < len(UNITS):
            start(*UNITS[unit + AHEAD])
        if unit == 2:
            filled(square_b, square_recv.at[1])
            total = square_c[...]
            for dz in range(1, NZ):
                total = total + square_b[dz - 1]
            for own_layer in range(2):
                trace = jnp.sum(total[own_layer], keepdims=True) * (1.0 / (tokens * width))
                level[own_layer] = jnp.broadcast_to(trace, (8, B)) * damping_ref[own_layer]

            @pl.when(has_before)
            def _():
                send(
                    level.at[0], level_next, level_sem.at[0], level_sem.at[1], before, dp
                ).start()

    filled(got, part_recv)
    for which in range(2):
        total = got[0, which]
        for step in range(1, NZ):
            total = total + got[step, which]
        reduced[which] = total * (1.0 / tokens)
    layer_here = jnp.where(keeps, upper, 1 - upper)
    moves = send(
        reduced, moved, move_sem.at[0], move_sem.at[1], section, at(across, x, beside)
    )
    follows = send(
        reduced.at[0],
        follow,
        follow_sem.at[0],
        follow_sem.at[1],
        jnp.where(layer_here == 0, before, section),
        at(jnp.where(keeps, across, y), x, jnp.where(keeps, z, beside)),
    )
    first_of_all = jnp.logical_not(has_before) & (layer_here == 0)
    last_of_all = jnp.logical_not(has_after) & (upper == 1)

    @pl.when(jnp.logical_not(first_of_all))
    def _():
        follows.start()

    @pl.when(jnp.logical_not(keeps))
    def _():
        moves.start()

    @pl.when(has_after)
    def _():
        filled(level_next, level_sem.at[1])

    @pl.when(upper == 0)
    def _():
        level_ref[0] = level[0]
        level_ref[1] = level[1]

    @pl.when((upper == 1) & has_after)
    def _():
        level_ref[0] = level[1]
        level_ref[1] = level_next[...]

    @pl.when(last_of_all)
    def _():
        level_ref[0] = level[1]
        level_ref[1] = jnp.zeros((8, B), jnp.float32)

    for piece in range(PIECES):
        for layer in range(2):
            for which in range(2):
                remote, _, own = item(piece, layer, which)
                started = jnp.logical_not(own)
                if (layer, which) == (1, 1) and piece in LENT:
                    started = started & jnp.logical_not(lends)
                pl.when(started)(remote.wait_send)
        pl.when(passes(piece))(passing(piece).wait_send)
    for piece in LENT:
        pl.when(lends)(lending(piece).wait_send)
        pl.when(borrows)(returning(piece).wait_send)
    sent = raw.at[:, :, pl.ds(1, len(PEERS))]
    filled(sent, raw_send)
    filled(square_a, square_send.at[0])
    filled(square_b, square_send.at[1])

    @pl.when(has_before)
    def _():
        filled(level_next, level_sem.at[0])

    @pl.when(keeps)
    def _():
        diagonal_ref[...] = reduced[0]
        cross_ref[...] = reduced[1]

    @pl.when(jnp.logical_not(keeps))
    def _():
        filled(moved, move_sem.at[1])
        diagonal_ref[...] = moved[0]
        cross_ref[...] = moved[1]

    @pl.when(last_of_all)
    def _():
        following_ref[...] = (
            lax.broadcasted_iota(jnp.int32, (B, B), 0) == lax.broadcasted_iota(jnp.int32, (B, B), 1)
        ).astype(jnp.float32)
        cross_ref[...] = jnp.zeros((B, B), jnp.float32)

    @pl.when(jnp.logical_not(last_of_all))
    def _():
        filled(follow, follow_sem.at[1])
        following_ref[...] = follow[...]

    @pl.when(jnp.logical_not(keeps))
    def _():
        filled(moved, move_sem.at[0])

    @pl.when(jnp.logical_not(first_of_all))
    def _():
        filled(follow, follow_sem.at[0])


def local(activations, damping):
    rows, layers, width = activations.shape
    tokens = rows * lax.axis_size("dp")
    depth = len(PEERS) + 1
    f32, bf16 = jnp.float32, jnp.bfloat16
    vmem = pl.BlockSpec(memory_space=pltpu.VMEM)
    block = jax.ShapeDtypeStruct((B, B), f32)
    diagonal, cross, following, level = pl.pallas_call(
        functools.partial(gram_kernel, tokens),
        out_shape=(block, block, block, jax.ShapeDtypeStruct((2, 8, B), f32)),
        in_specs=[pl.BlockSpec(memory_space=pl.ANY), pl.BlockSpec(memory_space=pltpu.SMEM)],
        out_specs=(vmem,) * 4,
        scratch_shapes=[
            pltpu.VMEM((rows, layers, width), bf16),
            pltpu.VMEM((layers, width // B, rows, B), bf16),
            pltpu.VMEM((PIECES, 2, depth, rows, B), bf16),
            pltpu.VMEM((PIECES, depth, rows, B), bf16),
            pltpu.VMEM((len(LENT), depth, rows, B), bf16),
            pltpu.VMEM((PIECES, 2, 2, B, B), f32),
            pltpu.VMEM((len(LENT), B, B), f32),
            pltpu.VMEM((NZ, 2, B, B), f32),
            pltpu.VMEM((2, B, B), f32),
            pltpu.VMEM((2, B, B), f32),
            pltpu.VMEM((B, B), f32),
            pltpu.VMEM((2, 8, B), f32),
            pltpu.VMEM((len(PEERS), 2, 8, B), f32),
            pltpu.VMEM((NZ - 1, 2, 8, B), f32),
            pltpu.VMEM((2, 8, B), f32),
            pltpu.VMEM((2, 8, B), f32),
            pltpu.VMEM((8, B), f32),
            pltpu.SemaphoreType.DMA,
            pltpu.SemaphoreType.DMA,
            pltpu.SemaphoreType.DMA((PIECES, 2)),
            pltpu.SemaphoreType.DMA((PIECES,)),
            pltpu.SemaphoreType.DMA((PIECES,)),
            pltpu.SemaphoreType.DMA((len(LENT),)),
            pltpu.SemaphoreType.DMA((len(LENT),)),
            pltpu.SemaphoreType.DMA((len(LENT),)),
            pltpu.SemaphoreType.DMA((PIECES, 2, 2)),
            pltpu.SemaphoreType.DMA,
            pltpu.SemaphoreType.DMA((2,)),
            pltpu.SemaphoreType.DMA((2,)),
            pltpu.SemaphoreType.DMA((2,)),
            pltpu.SemaphoreType.DMA((2,)),
            pltpu.SemaphoreType.DMA((2,)),
        ],
        compiler_params=pltpu.CompilerParams(
            collective_id=0, has_side_effects=True, vmem_limit_bytes=123 * 2**19
        ),
        name="grams",
    )(activations, damping)
    result = jax.ShapeDtypeStruct((1, B, B), f32)
    return pl.pallas_call(
        solve_kernel,
        out_shape=(result, result),
        name="solve",
    )(diagonal, cross, following, level)


def solution(mesh):
    placed = (P("dp", "section", None), P("section"))
    return jax.shard_map(
        local,
        mesh=mesh,
        in_specs=placed,
        out_specs=(P(("section", "dp"), None, None), P(("section", "dp"), None, None)),
        check_vma=False,
    )
```

```python
import functools

import jax
import jax.numpy as jnp
from jax import lax
from jax.experimental import pallas as pl
from jax.experimental.pallas import tpu as pltpu
from jax.sharding import PartitionSpec as P

MESH = pl.DeviceIdType.MESH
HIGHEST = lax.Precision.HIGHEST
B = 128
W = 16
NY, NX, NZ = 4, 2, 8
PIECES = 4
PEERS = ((0, 1), (1, 0), (3, 0), (1, 1), (3, 1), (2, 0), (2, 1))
TURN = (2, 1, 3, 0)
LENT = (0, 2)
LATER = 3
SQUARES = (2, 4)
AHEAD = 4
UNITS = tuple((piece, layer) for piece in range(PIECES) for layer in range(2))


def product(a, b):
    return lax.dot_general(
        a, b, (((1,), (0,)), ((), ())), precision=HIGHEST, preferred_element_type=jnp.float32
    )


def product_t(a, b):
    return lax.dot_general(
        a, b, (((1,), (1,)), ((), ())), precision=HIGHEST, preferred_element_type=jnp.float32
    )


def gram(a, b):
    return lax.dot_general(a, b, (((0,), (0,)), ((), ())), preferred_element_type=jnp.float32)


def small_inverse(panel, first):
    row = lax.broadcasted_iota(jnp.int32, (8, B), 0)
    halves = [panel[8 * h : 8 * h + 8] for h in range(W // 8)]
    columns = [
        [jnp.broadcast_to(half[:, first + j : first + j + 1], (8, B)) for half in halves]
        for j in range(W)
    ]
    for j in range(W):
        h, i = divmod(j, 8)
        own = row == i
        pivot = columns[j]
        inverse = 1.0 / pivot[h][i : i + 1]
        for k in range(W):
            if k == j:
                continue
            scaled = columns[k][h][i : i + 1] * inverse
            new = [c - p * scaled for c, p in zip(columns[k], pivot)]
            new[h] = jnp.where(own, scaled, new[h])
            columns[k] = new
        new = [-p * inverse for p in pivot]
        new[h] = jnp.where(own, inverse, new[h])
        columns[j] = new
    return columns


def invert(a):
    lane = lax.broadcasted_iota(jnp.int32, (B, B), 1)
    row = lax.broadcasted_iota(jnp.int32, (W, B), 0)
    panel = a[:W]
    for first in range(0, B, W):
        last = first + W
        columns = small_inverse(panel, first)
        inside = (lane >= first) & (lane < last)
        identity = (lane[:W] - first == row).astype(jnp.float32)
        panel = jnp.where(inside[:W], identity, panel)
        halves = []
        for h in range(W // 8):
            total = columns[0][h] * panel[0:1]
            for j in range(1, W):
                total = total + columns[j][h] * panel[j : j + 1]
            halves.append(total)
        rows = jnp.concatenate(halves, axis=0)
        halves = []
        for h in range(W // 8 if last < B else 0):
            below = a[last + 8 * h : last + 8 * h + 8]
            total = jnp.where(inside[:8], 0.0, below)
            for j in range(W):
                factor = jnp.broadcast_to(below[:, first + j : first + j + 1], (8, B))
                total = total - factor * rows[j : j + 1]
            halves.append(total)
        if halves:
            panel = jnp.concatenate(halves, axis=0)
        rest = jnp.where(inside, 0.0, a) - product(a[:, first:last], rows)
        parts = [rest[:first]] if first else []
        parts.append(rows)
        if last < B:
            parts.append(rest[last:])
        a = jnp.concatenate(parts, axis=0)
    return a


def solve_kernel(diagonal_ref, cross_ref, following_ref, level_ref, inverse_ref, coupling_ref):
    diagonal = lax.broadcasted_iota(jnp.int32, (B, B), 0) == lax.broadcasted_iota(
        jnp.int32, (B, B), 1
    )
    cross = cross_ref[...]
    following = following_ref[...]
    following = jnp.where(diagonal, following + level_ref[1, 0:1, :], following)
    coupling = product(cross, invert(following))
    coupling_ref[0] = coupling
    damped = diagonal_ref[...]
    damped = jnp.where(diagonal, damped + level_ref[0, 0:1, :], damped)
    inverse_ref[0] = invert(damped - product_t(coupling, cross))


def filled(ref, semaphore):
    pltpu.make_async_copy(ref, ref, semaphore).wait()


def gram_kernel(
    tokens,
    x_hbm,
    damping_ref,
    diagonal_ref,
    cross_ref,
    following_ref,
    level_ref,
    mixed,
    x_ref,
    raw,
    passed,
    lent,
    partial,
    returned,
    got,
    reduced,
    moved,
    follow,
    square,
    square_a,
    square_b,
    square_c,
    level,
    level_next,
    load_sem,
    raw_send,
    raw_recv,
    pass_send,
    pass_recv,
    lend_send,
    lend_recv,
    return_send,
    part_send,
    part_recv,
    move_sem,
    follow_sem,
    square_send,
    square_recv,
    level_sem,
):
    section, dp = lax.axis_index("section"), lax.axis_index("dp")
    sections = lax.axis_size("section")
    y, x, z = dp // (NX * NZ), (dp // NZ) % NX, dp % NZ
    upper = y // 2
    has_before, has_after = section > 0, section < sections - 1
    lends, borrows = section == sections // 2 - 1, section == sections // 2
    before, after = lax.rem(section + sections - 1, sections), lax.rem(section + 1, sections)
    across = lax.rem(y + 2, NY)
    beside = z + 1 - 2 * lax.rem(z, 2)
    keeps = lax.rem(z, 2) == upper

    def at(y, x, z):
        return y * (NX * NZ) + x * NZ + z

    def near(dy, dx):
        return lax.rem(y + dy, NY), lax.rem(x + dx, NX)

    def send(src, dst, send_sem, recv_sem, to_section, to_dp):
        return pltpu.make_async_remote_copy(
            src_ref=src,
            dst_ref=dst,
            send_sem=send_sem,
            recv_sem=recv_sem,
            device_id=(to_section, to_dp),
            device_id_type=MESH,
        )

    load = pltpu.make_async_copy(x_hbm, mixed, load_sem)
    load.start()
    barrier = pltpu.get_barrier_semaphore()
    greeted = [(section, at(*near(dy, dx), z)) for dy, dx in PEERS]
    for dz in range(1, NZ):
        other = lax.rem(z + dz, NZ)
        greeted += [(to_section, at(y, x, other)) for to_section in (before, section, after)]
    greeted += [(before, dp), (after, dp), (section, at(across, x, beside))]
    greeted += [(before, at(across, x, z)), (after, at(across, x, z))]
    for device in greeted:
        pl.semaphore_signal(barrier, inc=1, device_id=device, device_id_type=MESH)
    def order(piece):
        return lax.rem(z // 2 + TURN[piece], PIECES)

    def block_of(piece, y, x):
        return (y % 2) * (NX * NZ) + x * NZ + y // 2 + 2 * order(piece)

    def source(piece, layer, y, x):
        return x_ref.at[layer, block_of(piece, y, x)]

    rows, layers, width = mixed.shape
    part = rows // 2
    picked = lax.broadcasted_iota(jnp.int32, (layers * part, layers * part), 0)
    place = lax.broadcasted_iota(jnp.int32, (layers * part, layers * part), 1)
    picked = layers * (picked % part) + picked // part == place
    picked = picked.astype(jnp.bfloat16)

    def by_layer(piece):
        blocks = [block_of(piece, y, x) for y in range(NY) for x in range(NX)]
        for top in range(0, rows, part):
            both = jnp.concatenate(
                [
                    mixed[top : top + part, :, pl.ds(pl.multiple_of(block * B, B), B)]
                    for block in blocks
                ],
                axis=2,
            ).reshape(layers * part, len(blocks) * B)
            apart = lax.dot_general(
                picked, both, (((1,), (0,)), ((), ())), preferred_element_type=jnp.float32
            ).astype(jnp.bfloat16)
            for layer in range(layers):
                for i, block in enumerate(blocks):
                    x_ref[layer, block, top : top + part, :] = apart[
                        layer * part : (layer + 1) * part, i * B : (i + 1) * B
                    ]

    def start(piece, layer):
        pltpu.make_async_copy(
            source(piece, layer, y, x), raw.at[piece, layer, 0], raw_recv.at[piece, layer]
        ).start()
        for slot, (dy, dx) in enumerate(PEERS, 1):
            to_y, to_x = near(dy, dx)
            send(
                source(piece, layer, to_y, to_x),
                raw.at[piece, layer, slot],
                raw_send,
                raw_recv.at[piece, layer],
                section,
                at(to_y, to_x, z),
            ).start()

    load.wait()
    by_layer(0)
    pl.semaphore_wait(barrier, len(greeted))
    start(*UNITS[0])
    by_layer(1)
    start(*UNITS[1])
    start(*UNITS[2])
    by_layer(2)
    by_layer(3)

    def add_block(block, totals):
        out = []
        for layer in range(2):
            total = totals[layer]
            for top in range(0, rows, 16):
                value = x_ref[layer, block, top : top + 16, :].astype(jnp.float32)
                total = total + value * value
            out.append(total)
        return tuple(out)

    zero = jnp.zeros((16, B), jnp.float32)
    totals = lax.fori_loop(0, width // B, add_block, (zero, zero))
    for layer in range(2):
        square[layer] = totals[layer][:8] + totals[layer][8:]
    for slot, (dy, dx) in enumerate(PEERS):
        to_y, to_x = near(dy, dx)
        send(
            square, square_a.at[slot], square_send.at[0], square_recv.at[0], section, at(to_y, to_x, z)
        ).start()
    for piece, layer in UNITS[3:AHEAD]:
        start(piece, layer)

    def target(piece, layer):
        to_z = 2 * order(piece) + layer
        return at(y, x, to_z), to_z == z

    def item(piece, layer, which):
        to_dp, own = target(piece, layer)
        src, dst = partial.at[piece, layer, which], got.at[which, z]
        remote = send(src, dst, part_send.at[piece, layer, which], part_recv.at[which], section, to_dp)
        local = pltpu.make_async_copy(src, dst, part_recv.at[which])
        return remote, local, own

    def deliver(piece, layer, which):
        remote, local, own = item(piece, layer, which)

        @pl.when(own)
        def _():
            local.start()

        @pl.when(jnp.logical_not(own))
        def _():
            remote.start()

    def passing(piece):
        return send(
            raw.at[piece, 0], passed.at[piece], pass_send.at[piece], pass_recv.at[piece], before, dp
        )

    def lending(piece):
        slot = LENT.index(piece)
        return send(
            raw.at[piece, 1], lent.at[slot], lend_send.at[slot], lend_recv.at[slot], after, dp
        )

    def returning(piece):
        slot = LENT.index(piece)
        return send(
            returned.at[slot],
            got.at[1, z],
            return_send.at[slot],
            part_recv.at[1],
            before,
            target(piece, 1)[0],
        )

    def passes(piece):
        return has_before & jnp.logical_not(borrows) if piece in LENT else has_before

    def receives(piece):
        return has_after & jnp.logical_not(lends) if piece in LENT else has_after

    depth = len(PEERS) + 1

    def columns(ref):
        return ref[...].reshape(depth * rows, B)

    for unit, (piece, layer) in enumerate(UNITS):
        filled(raw.at[piece, layer], raw_recv.at[piece, layer])
        if layer == 0:
            pl.when(passes(piece))(passing(piece).start)
            first = columns(raw.at[piece, 0])
            partial[piece, 0, 0] = gram(first, first)
            deliver(piece, 0, 0)
        else:
            if piece in LENT:
                pl.when(lends)(lending(piece).start)
            first, second = columns(raw.at[piece, 0]), columns(raw.at[piece, 1])
            partial[piece, 1, 0] = gram(second, second)
            deliver(piece, 1, 0)
            partial[piece, 0, 1] = gram(first, second)
            deliver(piece, 0, 1)

            @pl.when(receives(piece))
            def _():
                filled(passed.at[piece], pass_recv.at[piece])
                partial[piece, 1, 1] = gram(second, columns(passed.at[piece]))
                deliver(piece, 1, 1)

            @pl.when(jnp.logical_not(has_after))
            def _():
                partial[piece, 1, 1] = jnp.zeros((B, B), jnp.float32)
                deliver(piece, 1, 1)

        for slot, borrowed in enumerate(LENT):
            if unit == 2 * borrowed + LATER:

                @pl.when(borrows)
                def _():
                    filled(lent.at[slot], lend_recv.at[slot])
                    returned[slot] = gram(columns(lent.at[slot]), columns(raw.at[borrowed, 0]))
                    returning(borrowed).start()

        if unit + AHEAD < len(UNITS):
            start(*UNITS[unit + AHEAD])
        if unit == SQUARES[0]:
            filled(square_a, square_recv.at[0])
            total = square[...]
            for slot in range(len(PEERS)):
                total = total + square_a[slot]
            square_c[...] = total
            for dz in range(1, NZ):
                send(
                    square_c,
                    square_b.at[dz - 1],
                    square_send.at[1],
                    square_recv.at[1],
                    section,
                    at(y, x, lax.rem(z + dz, NZ)),
                ).start()
        if unit == SQUARES[1]:
            filled(square_b, square_recv.at[1])
            total = square_c[...]
            for dz in range(1, NZ):
                total = total + square_b[dz - 1]
            for own_layer in range(2):
                trace = jnp.sum(total[own_layer], keepdims=True) * (1.0 / (tokens * width))
                level[own_layer] = jnp.broadcast_to(trace, (8, B)) * damping_ref[own_layer]

            @pl.when(has_before)
            def _():
                send(
                    level.at[0], level_next, level_sem.at[0], level_sem.at[1], before, dp
                ).start()

    layer_here = jnp.where(keeps, upper, 1 - upper)
    moves = [
        send(
            reduced.at[which],
            moved.at[which],
            move_sem.at[0, which],
            move_sem.at[1, which],
            section,
            at(across, x, beside),
        )
        for which in range(2)
    ]
    follows = send(
        reduced.at[0],
        follow,
        follow_sem.at[0],
        follow_sem.at[1],
        jnp.where(layer_here == 0, before, section),
        at(jnp.where(keeps, across, y), x, jnp.where(keeps, z, beside)),
    )
    first_of_all = jnp.logical_not(has_before) & (layer_here == 0)
    last_of_all = jnp.logical_not(has_after) & (upper == 1)

    for which in range(2):
        filled(got.at[which], part_recv.at[which])
        total = got[which, 0]
        for step in range(1, NZ):
            total = total + got[which, step]
        reduced[which] = total * (1.0 / tokens)
        if which == 0:
            pl.when(jnp.logical_not(first_of_all))(follows.start)
        pl.when(jnp.logical_not(keeps))(moves[which].start)

    @pl.when(has_after)
    def _():
        filled(level_next, level_sem.at[1])

    @pl.when(upper == 0)
    def _():
        level_ref[0] = level[0]
        level_ref[1] = level[1]

    @pl.when((upper == 1) & has_after)
    def _():
        level_ref[0] = level[1]
        level_ref[1] = level_next[...]

    @pl.when(last_of_all)
    def _():
        level_ref[0] = level[1]
        level_ref[1] = jnp.zeros((8, B), jnp.float32)

    for piece in range(PIECES):
        for layer in range(2):
            for which in range(2):
                remote, _, own = item(piece, layer, which)
                started = jnp.logical_not(own)
                if (layer, which) == (1, 1) and piece in LENT:
                    started = started & jnp.logical_not(lends)
                pl.when(started)(remote.wait_send)
        pl.when(passes(piece))(passing(piece).wait_send)
    for piece in LENT:
        pl.when(lends)(lending(piece).wait_send)
        pl.when(borrows)(returning(piece).wait_send)
    sent = raw.at[:, :, pl.ds(1, len(PEERS))]
    filled(sent, raw_send)
    filled(square_a, square_send.at[0])
    filled(square_b, square_send.at[1])

    @pl.when(has_before)
    def _():
        filled(level_next, level_sem.at[0])

    @pl.when(keeps)
    def _():
        diagonal_ref[...] = reduced[0]
        cross_ref[...] = reduced[1]

    @pl.when(jnp.logical_not(keeps))
    def _():
        for which in range(2):
            filled(moved.at[which], move_sem.at[1, which])
        diagonal_ref[...] = moved[0]
        cross_ref[...] = moved[1]

    @pl.when(last_of_all)
    def _():
        following_ref[...] = (
            lax.broadcasted_iota(jnp.int32, (B, B), 0) == lax.broadcasted_iota(jnp.int32, (B, B), 1)
        ).astype(jnp.float32)
        cross_ref[...] = jnp.zeros((B, B), jnp.float32)

    @pl.when(jnp.logical_not(last_of_all))
    def _():
        filled(follow, follow_sem.at[1])
        following_ref[...] = follow[...]

    @pl.when(jnp.logical_not(keeps))
    def _():
        for which in range(2):
            filled(moved.at[which], move_sem.at[0, which])

    @pl.when(jnp.logical_not(first_of_all))
    def _():
        filled(follow, follow_sem.at[0])


def local(activations, damping):
    rows, layers, width = activations.shape
    tokens = rows * lax.axis_size("dp")
    depth = len(PEERS) + 1
    f32, bf16 = jnp.float32, jnp.bfloat16
    vmem = pl.BlockSpec(memory_space=pltpu.VMEM)
    block = jax.ShapeDtypeStruct((B, B), f32)
    diagonal, cross, following, level = pl.pallas_call(
        functools.partial(gram_kernel, tokens),
        out_shape=(block, block, block, jax.ShapeDtypeStruct((2, 8, B), f32)),
        in_specs=[pl.BlockSpec(memory_space=pl.ANY), pl.BlockSpec(memory_space=pltpu.SMEM)],
        out_specs=(vmem,) * 4,
        scratch_shapes=[
            pltpu.VMEM((rows, layers, width), bf16),
            pltpu.VMEM((layers, width // B, rows, B), bf16),
            pltpu.VMEM((PIECES, 2, depth, rows, B), bf16),
            pltpu.VMEM((PIECES, depth, rows, B), bf16),
            pltpu.VMEM((len(LENT), depth, rows, B), bf16),
            pltpu.VMEM((PIECES, 2, 2, B, B), f32),
            pltpu.VMEM((len(LENT), B, B), f32),
            pltpu.VMEM((2, NZ, B, B), f32),
            pltpu.VMEM((2, B, B), f32),
            pltpu.VMEM((2, B, B), f32),
            pltpu.VMEM((B, B), f32),
            pltpu.VMEM((2, 8, B), f32),
            pltpu.VMEM((len(PEERS), 2, 8, B), f32),
            pltpu.VMEM((NZ - 1, 2, 8, B), f32),
            pltpu.VMEM((2, 8, B), f32),
            pltpu.VMEM((2, 8, B), f32),
            pltpu.VMEM((8, B), f32),
            pltpu.SemaphoreType.DMA,
            pltpu.SemaphoreType.DMA,
            pltpu.SemaphoreType.DMA((PIECES, 2)),
            pltpu.SemaphoreType.DMA((PIECES,)),
            pltpu.SemaphoreType.DMA((PIECES,)),
            pltpu.SemaphoreType.DMA((len(LENT),)),
            pltpu.SemaphoreType.DMA((len(LENT),)),
            pltpu.SemaphoreType.DMA((len(LENT),)),
            pltpu.SemaphoreType.DMA((PIECES, 2, 2)),
            pltpu.SemaphoreType.DMA((2,)),
            pltpu.SemaphoreType.DMA((2, 2)),
            pltpu.SemaphoreType.DMA((2,)),
            pltpu.SemaphoreType.DMA((2,)),
            pltpu.SemaphoreType.DMA((2,)),
            pltpu.SemaphoreType.DMA((2,)),
        ],
        compiler_params=pltpu.CompilerParams(
            collective_id=0, has_side_effects=True, vmem_limit_bytes=123 * 2**19
        ),
        name="grams",
    )(activations, damping)
    result = jax.ShapeDtypeStruct((1, B, B), f32)
    return pl.pallas_call(
        solve_kernel,
        out_shape=(result, result),
        name="solve",
    )(diagonal, cross, following, level)


def solution(mesh):
    placed = (P("dp", "section", None), P("section"))
    return jax.shard_map(
        local,
        mesh=mesh,
        in_specs=placed,
        out_specs=(P(("section", "dp"), None, None), P(("section", "dp"), None, None)),
        check_vma=False,
    )
```
